32 devices in a mesh: dp: 4 (over y, z), tp: 8 (over x, core).
Axes of the slice: x: 4, y: 2, z: 2, core: 2. Of those that a mesh axis runs over, the one named last changes fastest.
The devices are a block of a 4x4x8 slice.
Arguments:
- enc_out: bfloat16 [512, 192, 512], P('dp'), parts along dimension 0
- w_proj: bfloat16 [512, 1024], P(None, 'tp')
- labels: int32 [512, 48], P('dp'), parts along dimension 0
- in_len: int32 [512], P('dp'), parts along dimension 0
- lab_len: int32 [512], P('dp'), parts along dimension 0
Outputs:
- output 1: float32 [512], P('dp'), parts along dimension 0
- output 2: float32 [2048, 1024], P('dp', 'tp'), parts along dimension 0
- output 3: float32 [512, 192, 512], P('dp'), parts along dimension 0
There are 4 independent parts. The reference program is written for one: setup_inputs(seed, part) draws one part's arguments, and reference() takes and returns one part's arrays. A program takes and returns all parts, laid end to end along the dimension named above; an argument that names none is the same for every part.
All inputs are finite; a program needn't handle non-finite values.
Results may differ from the reference program's by a relative error of at most 0.001.
Values are sent between devices in bfloat16 or wider.
A program may use at most 768 MiB of HBM per device.

```python
import math
import jax
import jax.numpy as jnp
from jax import lax

HIDDEN = 512
VOCAB = 1024
FRAMES = 192
MAX_LABELS = 48
BATCH = 128
LAB_MIN = max(1, MAX_LABELS // 5)
NEG_FILL = -1.0e30


def draw_targets(int_key):
    key_lab, key_len, key_in, key_pos = jax.random.split(int_key, 4)
    seq_ids = jnp.arange(BATCH)
    full_pos = jax.random.randint(key_pos, (), 0, BATCH)
    tight_pos = (full_pos + BATCH // 2) % BATCH
    lab_len = jax.random.randint(key_len, (BATCH,), LAB_MIN, MAX_LABELS + 1)
    lab_len = jnp.where(seq_ids == full_pos, MAX_LABELS, jnp.where(seq_ids == tight_pos, LAB_MIN, lab_len))
    in_low = jnp.maximum(2 * lab_len + 1, FRAMES // 5)
    in_len = jax.random.randint(key_in, (BATCH,), in_low, FRAMES + 1)
    in_len = jnp.where(seq_ids == full_pos, FRAMES, jnp.where(seq_ids == tight_pos, 2 * LAB_MIN + 1, in_len))
    lab_ids = jnp.arange(MAX_LABELS)
    labels = jax.random.randint(key_lab, (BATCH, MAX_LABELS), 1, VOCAB)
    at_full = (seq_ids == full_pos)[:, None]
    labels = jnp.where(at_full & (lab_ids == 0)[None, :], 1, jnp.where(at_full & (lab_ids == MAX_LABELS - 1)[None, :], VOCAB - 1, labels))
    return labels.astype(jnp.int32), in_len.astype(jnp.int32), lab_len.astype(jnp.int32)


def setup_inputs(seed: int = 0, part: int = 0) -> dict:
    base_key = jax.random.key(seed)
    part_key = jax.random.fold_in(base_key, part)
    key_hs, key_int = jax.random.split(part_key, 2)
    key_w = jax.random.key(seed + 1)
    enc_out = jax.random.normal(key_hs, (BATCH, FRAMES, HIDDEN), jnp.float32).astype(jnp.bfloat16)
    w_proj = (jax.random.normal(key_w, (HIDDEN, VOCAB), jnp.float32) * (2.0 / math.sqrt(HIDDEN))).astype(jnp.bfloat16)
    labels, in_len, lab_len = draw_targets(key_int)
    return {"enc_out": enc_out, "w_proj": w_proj, "labels": labels, "in_len": in_len, "lab_len": lab_len}


def lattice_loss(label_lp, labels, in_len, lab_len):
    n_seq, n_frames, n_cols = label_lp.shape
    n_lab = n_cols - 1
    n_states = 2 * n_lab + 1
    blank_lp = label_lp[:, :, :1]
    interleaved = jnp.stack([jnp.broadcast_to(blank_lp, (n_seq, n_frames, n_lab)), label_lp[:, :, 1:]], axis=-1)
    emit_all = jnp.concatenate([interleaved.reshape(n_seq, n_frames, 2 * n_lab), blank_lp], axis=-1)
    emit_tm = jnp.swapaxes(emit_all, 0, 1)
    skip_lab = jnp.pad(labels[:, 1:] != labels[:, :-1], ((0, 0), (1, 0)))
    skip_ok = jnp.pad(jnp.stack([jnp.zeros_like(skip_lab), skip_lab], axis=-1).reshape(n_seq, 2 * n_lab), ((0, 0), (0, 1)))
    state_ids = jnp.arange(n_states)
    neg_one = jnp.full((n_seq, 1), NEG_FILL, label_lp.dtype)
    neg_two = jnp.full((n_seq, 2), NEG_FILL, label_lp.dtype)
    alpha_init = jnp.where(state_ids[None, :] == 0, 0.0, neg_one)

    def lattice_step(alpha_prev, step_in):
        emit_t, frame_idx = step_in
        prev_one = jnp.concatenate([neg_one, alpha_prev[:, :-1]], axis=1)
        prev_two = jnp.where(skip_ok, jnp.concatenate([neg_two, alpha_prev[:, :-2]], axis=1), NEG_FILL)
        top_val = lax.stop_gradient(jnp.maximum(jnp.maximum(alpha_prev, prev_one), prev_two))
        merged = top_val + jnp.log(jnp.exp(alpha_prev - top_val) + jnp.exp(prev_one - top_val) + jnp.exp(prev_two - top_val))
        live_seq = (frame_idx < in_len)[:, None]
        return jnp.where(live_seq, merged + emit_t, alpha_prev), None

    alpha_end, _ = lax.scan(lattice_step, alpha_init, (emit_tm, jnp.arange(n_frames)))
    end_sel = (state_ids[None, :] == 2 * lab_len[:, None]) | (state_ids[None, :] == 2 * lab_len[:, None] - 1)
    return -jax.nn.logsumexp(jnp.where(end_sel, alpha_end, NEG_FILL), axis=1)


def label_logprobs(logits, ext_seq):
    log_norm = jax.nn.logsumexp(logits, axis=-1)
    return jnp.take(logits, ext_seq, axis=1) - log_norm[:, None]


def reference(enc_out, w_proj, labels, in_len, lab_len):
    ext_all = jnp.concatenate([jnp.zeros((BATCH, 1), jnp.int32), labels], axis=1)

    def forward_seq(seq_in):
        enc_seq, ext_seq = seq_in
        logits = jnp.dot(enc_seq, w_proj, preferred_element_type=jnp.float32)
        return label_logprobs(logits, ext_seq)

    label_lp = lax.map(forward_seq, (enc_out, ext_all))
    loss, lattice_vjp = jax.vjp(lambda lp_in: lattice_loss(lp_in, labels, in_len, lab_len), label_lp)
    (lp_grad,) = lattice_vjp(jnp.ones_like(loss))

    def backward_seq(grad_acc, seq_in):
        enc_seq, ext_seq, cot_seq = seq_in
        logits = jnp.dot(enc_seq, w_proj, preferred_element_type=jnp.float32)
        _, lp_vjp = jax.vjp(lambda z_in: label_logprobs(z_in, ext_seq), logits)
        (grad_z,) = lp_vjp(cot_seq)
        grad_bf = grad_z.astype(jnp.bfloat16)
        grad_acc = grad_acc + jnp.dot(enc_seq.T, grad_bf, preferred_element_type=jnp.float32)
        grad_hs = jnp.dot(grad_bf, w_proj.T, preferred_element_type=jnp.float32)
        return grad_acc, grad_hs

    grad_w, grad_hs = lax.scan(backward_seq, jnp.zeros((HIDDEN, VOCAB), jnp.float32), (enc_out, ext_all, lp_grad))
    return loss, grad_w, grad_hs
```

```python
import functools

import jax
import jax.numpy as jnp
from jax import lax
from jax.experimental import pallas as pl
from jax.experimental.pallas import tpu as pltpu
from jax.sharding import PartitionSpec as P

NEG_FILL = -1.0e30
LANES = 128
SEQS = 8
ROWS = 32
VMEM_BYTES = 60 * 1024 * 1024


def dot(a, b):
    return jnp.dot(a, b, preferred_element_type=jnp.float32)


def column(table, index):
    lane = lax.broadcasted_iota(jnp.int32, table.shape, 1)
    return jnp.sum(jnp.where(lane == index, table, 0), axis=1, keepdims=True)


def for_live_rows(n_live, n_frames, body):
    n_steps = lax.div(n_live + (ROWS - 1), ROWS)
    for step in range(1, n_frames // ROWS + 1):
        @pl.when(n_steps == step)
        def _():
            body(step * ROWS)


def lattice_kernel(n_own, n_states, meta, in_len_s, enc_ref, w_ref, wt_ref, lab_ref, aux_ref,
                   occ_ref, loss_ref, w0_ref, w1_ref, w2_ref, z_ref, sel_ref):
    step = pl.program_id(0)
    n_frames = enc_ref.shape[1]
    n_lab = lab_ref.shape[0]
    n_cols = w_ref.shape[1]
    flat = occ_ref.reshape(n_frames * n_own, LANES)

    @pl.when(step == 0)
    def _():
        row = lax.broadcasted_iota(jnp.int32, (LANES, LANES), 0)
        for h in range(sel_ref.shape[0]):
            blank = wt_ref[0:1, h * LANES:(h + 1) * LANES].astype(jnp.float32)
            sel_ref[h] = jnp.where(row % 2 == 0, blank, 0.0)

    def one_seq(s, carry):
        local = step * SEQS + s
        seq = meta[0] * n_own + local
        labs = column(lab_ref[...], seq)
        cols = lax.broadcasted_iota(jnp.int32, (n_lab, n_cols), 1)
        one_hot = jnp.where(cols == labs, 1.0, 0.0).astype(jnp.bfloat16)
        picked = dot(one_hot, wt_ref[...])
        for h in range(sel_ref.shape[0]):
            sel_ref[h, pl.ds(1, n_lab, stride=2), :] = picked[:, h * LANES:(h + 1) * LANES]
        w_sel = jnp.concatenate([sel_ref[h] for h in range(sel_ref.shape[0])], axis=1).astype(jnp.bfloat16)

        def rows_body(rows):
            enc = enc_ref[s, :rows, :]
            z_ref[:rows, :] = dot(enc, w_ref[...])
            emit = lax.dot_general(enc, w_sel, (((1,), (1,)), ((), ())), preferred_element_type=jnp.float32)
            z = z_ref[:rows, :]
            top = jnp.max(z, axis=1, keepdims=True)
            lse = top + jnp.log(jnp.sum(jnp.exp(z - top), axis=1, keepdims=True))
            lane = lax.broadcasted_iota(jnp.int32, (rows, LANES), 1)
            flat[pl.ds(local, rows, stride=n_own), :] = jnp.where(lane == LANES - 1, lse, emit - lse)

        for_live_rows(in_len_s[seq], n_frames, rows_body)
        return carry

    lax.fori_loop(0, SEQS, one_seq, 0)

    @pl.when(step == pl.num_programs(0) - 1)
    def _():
        skip_ok = aux_ref[0] != 0
        in_len = aux_ref[1]
        end_sel = aux_ref[2] != 0
        lane = lax.broadcasted_iota(jnp.int32, (n_own, LANES), 1)
        valid = lane < n_states

        def forward(t, alpha):
            live = t < in_len
            one = pltpu.roll(alpha, 1, 1)
            two = jnp.where(skip_ok, pltpu.roll(alpha, 2, 1), NEG_FILL)
            top = jnp.maximum(jnp.maximum(alpha, one), two)
            e0 = jnp.exp(alpha - top)
            e1 = jnp.exp(one - top)
            e2 = jnp.exp(two - top)
            total = e0 + e1 + e2
            merged = top + jnp.log(total)
            inv = jnp.where(live, 1.0 / total, 0.0)
            w0_ref[t] = jnp.where(live, e0 * inv, 1.0)
            w1_ref[t] = e1 * inv
            w2_ref[t] = e2 * inv
            emit = jnp.where(valid, occ_ref[t], NEG_FILL)
            return jnp.where(live, merged + emit, alpha)

        alpha = lax.fori_loop(0, n_frames, forward, jnp.where(lane == 0, 0.0, NEG_FILL).astype(jnp.float32))
        ends = jnp.where(end_sel, alpha, NEG_FILL)
        top = jnp.max(ends, axis=1, keepdims=True)
        weight = jnp.where(end_sel, jnp.exp(ends - top), 0.0)
        total = jnp.sum(weight, axis=1, keepdims=True)
        loss_ref[...] = jnp.broadcast_to(-(top + jnp.log(total)), (n_own, LANES))

        def backward(i, post):
            t = n_frames - 1 - i
            live = t < in_len
            occ_ref[t] = jnp.where(lane == LANES - 1, occ_ref[t], jnp.where(live, post, 0.0))
            return (post * w0_ref[t] + pltpu.roll(post * w1_ref[t], LANES - 1, 1)) + pltpu.roll(post * w2_ref[t], LANES - 2, 1)

        lax.fori_loop(0, n_frames, backward, weight / total)


def grad_kernel(first, meta, in_len_s, enc_ref, w_ref, wt_ref, occ_ref, lab_ref, *rest):
    if first:
        hs_ref, gw_ref, g_ref, hot_ref, acc_ref = rest
    else:
        _, gw_in_ref, hs_ref, gw_ref, g_ref, hot_ref, acc_ref = rest
    step = pl.program_id(0)
    n_frames = enc_ref.shape[1]
    n_cols = w_ref.shape[1]
    n_hid = w_ref.shape[0]
    n_chunk = 256
    flat = occ_ref.reshape(n_frames * SEQS, LANES)

    @pl.when(step == 0)
    def _():
        acc_ref[...] = jnp.zeros_like(acc_ref)

    def one_seq(s, carry):
        seq = (meta[0] * pl.num_programs(0) + step) * SEQS + s
        n_live = in_len_s[seq]
        labs = column(lab_ref[...], seq)
        cols = lax.broadcasted_iota(jnp.int32, (labs.shape[0], n_cols), 1)
        hot_ref[...] = jnp.where(cols == labs, 1.0, 0.0).astype(jnp.bfloat16)

        def rows_body(rows):
            enc = enc_ref[s, :rows, :]
            occ = flat[pl.ds(s, rows, stride=SEQS), :]
            lane = lax.broadcasted_iota(jnp.int32, (rows, LANES), 1)
            odd = lane % 2 == 1
            lse = occ[:, LANES - 1:]
            states = jnp.where(lane < LANES - 1, occ, 0.0)
            blank = jnp.sum(jnp.where(odd, 0.0, states), axis=1, keepdims=True)
            value = jnp.where(odd, states, blank)
            high = value.astype(jnp.bfloat16).astype(jnp.float32)
            rest1 = value - high
            mid = rest1.astype(jnp.bfloat16).astype(jnp.float32)
            low = rest1 - mid
            part_a = jnp.where(odd, high, pltpu.roll(mid, LANES - 1, 1))
            part_b = jnp.where(odd | (lane == 4), low, jnp.where(lane == 0, high, mid))
            parts = jnp.concatenate([part_a, part_b], axis=1).astype(jnp.bfloat16)
            frame = lax.broadcasted_iota(jnp.int32, (rows, n_chunk), 0)
            live = frame < n_live
            for c in range(0, n_cols, n_chunk):
                prob = jnp.exp(dot(enc, w_ref[:, c:c + n_chunk]) - lse)
                spread = dot(parts, hot_ref[:, c:c + n_chunk])
                g_ref[:rows, c:c + n_chunk] = jnp.where(live, prob - spread, 0.0).astype(jnp.bfloat16)
            hs_ref[s, :rows, :] = dot(g_ref[:rows, :], wt_ref[...])
            if rows < n_frames:
                hs_ref[s, rows:, :] = jnp.zeros((n_frames - rows, n_hid), jnp.float32)
            mine = g_ref[:rows, pl.ds(pl.multiple_of(meta[1] * LANES, LANES), LANES)]
            acc_ref[...] += lax.dot_general(mine, enc, (((0,), (0,)), ((), ())), preferred_element_type=jnp.float32)

        for_live_rows(n_live, n_frames, rows_body)
        return carry

    lax.fori_loop(0, SEQS, one_seq, 0)

    @pl.when(step == pl.num_programs(0) - 1)
    def _():
        total = acc_ref[...].T
        gw_ref[...] = total if first else total + gw_in_ref[...]


def run_lattice(meta, in_len, enc_out, w_all, wt_all, lab_t, aux, n_own, n_states):
    n_frames, n_hid = enc_out.shape[1:]
    n_cols = w_all.shape[1]
    n_step = n_own // SEQS
    whole = lambda *dims: pl.BlockSpec(dims, lambda i, m, l: (0,) * len(dims))
    return pl.pallas_call(
        functools.partial(lattice_kernel, n_own, n_states),
        grid_spec=pltpu.PrefetchScalarGridSpec(
            num_scalar_prefetch=2,
            grid=(n_step,),
            in_specs=[
                pl.BlockSpec((SEQS, n_frames, n_hid), lambda i, m, l: (m[0] * n_step + i, 0, 0)),
                whole(n_hid, n_cols),
                whole(n_cols, n_hid),
                whole(*lab_t.shape),
                pl.BlockSpec((3, n_own, LANES), lambda i, m, l: (0, m[0], 0)),
            ],
            out_specs=[whole(n_frames, n_own, LANES), whole(n_own, LANES)],
            scratch_shapes=[pltpu.VMEM((n_frames, n_own, LANES), jnp.float32)] * 3
            + [pltpu.VMEM((n_frames, n_cols), jnp.float32), pltpu.VMEM((n_hid // LANES, LANES, LANES), jnp.float32)],
        ),
        out_shape=[
            jax.ShapeDtypeStruct((n_frames, n_own, LANES), jnp.float32),
            jax.ShapeDtypeStruct((n_own, LANES), jnp.float32),
        ],
        compiler_params=pltpu.CompilerParams(vmem_limit_bytes=VMEM_BYTES),
        name="lattice",
    )(meta, in_len, enc_out, w_all, wt_all, lab_t, aux)


def run_grad(meta, in_len, enc_out, w_all, wt_all, occ, lab_cols, n_local, prior=None):
    n_batch, n_frames, n_hid = enc_out.shape
    n_cols = w_all.shape[1]
    n_step = occ.shape[1] // SEQS
    first = prior is None
    whole = lambda *dims: pl.BlockSpec(dims, lambda i, m, l: (0,) * len(dims))
    in_specs = [
        pl.BlockSpec((SEQS, n_frames, n_hid), lambda i, m, l: (m[0] * n_step + i, 0, 0)),
        whole(n_hid, n_cols),
        whole(n_cols, n_hid),
        pl.BlockSpec((n_frames, SEQS, LANES), lambda i, m, l: (0, i, 0)),
        whole(*lab_cols.shape),
    ]
    operands = [meta, in_len, enc_out, w_all, wt_all, occ, lab_cols]
    aliases = {}
    if not first:
        in_specs += [pl.BlockSpec(memory_space=pl.ANY), whole(n_hid, n_local)]
        operands += list(prior)
        aliases = {7: 0}
    return pl.pallas_call(
        functools.partial(grad_kernel, first),
        grid_spec=pltpu.PrefetchScalarGridSpec(
            num_scalar_prefetch=2,
            grid=(n_step,),
            in_specs=in_specs,
            out_specs=[
                pl.BlockSpec((SEQS, n_frames, n_hid), lambda i, m, l: (m[0] * n_step + i, 0, 0)),
                whole(n_hid, n_local),
            ],
            scratch_shapes=[
                pltpu.VMEM((n_frames, n_cols), jnp.bfloat16),
                pltpu.VMEM((2 * LANES, n_cols), jnp.bfloat16),
                pltpu.VMEM((n_local, n_hid), jnp.float32),
            ],
        ),
        out_shape=[
            jax.ShapeDtypeStruct((n_batch, n_frames, n_hid), jnp.float32),
            jax.ShapeDtypeStruct((n_hid, n_local), jnp.float32),
        ],
        input_output_aliases=aliases,
        compiler_params=pltpu.CompilerParams(vmem_limit_bytes=VMEM_BYTES),
        cost_estimate=pl.CostEstimate(flops=2 * (n_batch // 2) * n_frames * n_hid * n_cols * 3, bytes_accessed=40_000_000, transcendentals=0),
        name="grad_first" if first else "grad_second",
    )(*operands)


def solution(mesh):
    n_group = mesh.shape["tp"]

    def device_fn(enc_out, w_loc, labels, in_len, lab_len):
        n_batch, n_frames, n_hid = enc_out.shape
        n_local = w_loc.shape[1]
        n_lab = labels.shape[1]
        n_states = 2 * n_lab + 1
        n_own = n_batch // 2
        index = lax.axis_index("tp").astype(jnp.int32)
        half = index % 2
        wt_all = lax.all_gather(w_loc.T, "tp", axis=0, tiled=True)
        w_all = wt_all.T

        state = jnp.arange(LANES)[None, :]
        skip_lab = jnp.pad(labels[:, 1:] != labels[:, :-1], ((0, 0), (1, 0))).astype(jnp.int32)
        skip = jnp.stack([jnp.zeros_like(skip_lab), skip_lab], axis=-1).reshape(n_batch, 2 * n_lab)
        skip = jnp.pad(skip, ((0, 0), (0, LANES - 2 * n_lab)))
        ends = ((state == 2 * lab_len[:, None]) | (state == 2 * lab_len[:, None] - 1)).astype(jnp.int32)
        aux = jnp.stack([skip, jnp.broadcast_to(in_len[:, None], (n_batch, LANES)), ends])

        pairs = jnp.pad(jnp.repeat(labels, 2, axis=1), ((0, 0), (0, LANES - 2 * n_lab)), constant_values=-1)
        second = jnp.where(state % 2 == 1, pairs, jnp.where(state <= 4, 0, -1))
        lab_cols = jnp.concatenate([pairs, second], axis=1).T

        meta = jnp.stack([half, index])
        occ, loss = run_lattice(meta, in_len, enc_out, w_all, wt_all, labels.T, aux, n_own, n_states)
        partner = [(i, i ^ 1) for i in range(n_group)]
        occ_other = lax.ppermute(occ, "tp", partner)
        loss_mine = loss[:, 0]
        loss_other = lax.ppermute(loss_mine, "tp", partner)
        loss_all = jnp.where(half == 0, jnp.concatenate([loss_mine, loss_other]), jnp.concatenate([loss_other, loss_mine]))
        prior = run_grad(meta, in_len, enc_out, w_all, wt_all, occ, lab_cols, n_local)
        grad_hs, grad_w = run_grad(jnp.stack([1 - half, index]), in_len, enc_out, w_all, wt_all, occ_other, lab_cols, n_local, prior)
        return loss_all, grad_w, grad_hs

    return jax.shard_map(device_fn, mesh=mesh, in_specs=(P("dp"), P(None, "tp"), P("dp"), P("dp"), P("dp")), out_specs=(P("dp"), P("dp", "tp"), P("dp")), check_vma=False)
```

```python
import functools

import jax
import jax.numpy as jnp
from jax import lax
from jax.experimental import pallas as pl
from jax.experimental.pallas import tpu as pltpu
from jax.sharding import PartitionSpec as P

NEG_FILL = -1.0e30
LANES = 128
SUBS = 8
GROUP = 4
ROWS = 32
VMEM_BYTES = 62 * 1024 * 1024
ORDER, LENGTH, SLOT, HALF, INDEX = range(5)


def dot(a, b):
    return jnp.dot(a, b, preferred_element_type=jnp.float32)


def column(table, index):
    lane = lax.broadcasted_iota(jnp.int32, table.shape, 1)
    return jnp.sum(jnp.where(lane == index, table, 0), axis=1, keepdims=True)


def one_hot_rows(labs, n_cols):
    cols = lax.broadcasted_iota(jnp.int32, (labs.shape[0], n_cols), 1)
    return jnp.where(cols == labs, 1.0, 0.0).astype(jnp.bfloat16)


def for_group_rows(info, first, n_frames, body):
    longest = info[LENGTH, first]
    for s in range(1, GROUP):
        longest = jnp.maximum(longest, info[LENGTH, first + s])
    n_steps = jnp.maximum(lax.div(longest + (ROWS - 1), ROWS), 2)
    for step in range(2, n_frames // ROWS + 1):
        @pl.when(n_steps == step)
        def _():
            body(step * ROWS)


def stack_rows(refs, rows):
    return jnp.concatenate([r[0, :rows, :] for r in refs], axis=0)


def lattice_kernel(n_own, info, *refs):
    enc_refs, refs = refs[:GROUP], refs[GROUP:]
    w_ref, lab_ref, side_ref, occ_hbm, wts, z_ref, pair_ref, lp_ref, aux_ref, out_sem = refs
    step = pl.program_id(0)
    n_frames = enc_refs[0].shape[1]
    n_lab = side_ref.shape[0] - 2 * SUBS
    n_cols = w_ref.shape[1]
    n_j = n_lab // SUBS
    n_pair, pitch = pair_ref.shape[:2]
    flat = pair_ref.reshape(n_pair * pitch, LANES)
    wide = LANES // 2

    first = info[HALF, 0] * n_own + step * GROUP

    def rows_body(rows):
        row = lax.broadcasted_iota(jnp.int32, (n_cols, LANES), 0)
        left = lax.broadcasted_iota(jnp.int32, (1, LANES), 1) < wide
        hots = []
        for s in range(0, GROUP, 2):
            labs = jnp.where(left, lab_ref[pl.ds(first + s, 1), :], lab_ref[pl.ds(first + s + 1, 1), :])
            hots.append(jnp.where(row == labs, 1.0, 0.0).astype(jnp.bfloat16))
        picked = dot(w_ref[...], jnp.concatenate(hots, axis=1)).astype(jnp.bfloat16)
        for s in range(GROUP):
            z_ref[s * rows:(s + 1) * rows, :] = dot(enc_refs[s][0, :rows, :], w_ref[...])
        emits = dot(stack_rows(enc_refs, rows), picked)
        lane = lax.broadcasted_iota(jnp.int32, (rows, LANES), 1) % wide
        for s in range(GROUP):
            half = emits[s * rows:(s + 1) * rows, s * wide:(s + 1) * wide]
            emit = jnp.concatenate([half, half], axis=1)
            z = z_ref[s * rows:(s + 1) * rows, :]
            top = jnp.max(z, axis=1, keepdims=True)
            lse = top + jnp.log(jnp.sum(jnp.exp(z - top), axis=1, keepdims=True))
            value = jnp.where(lane == n_lab + 1, lse, emit - lse)
            if rows > n_pair:
                both = jnp.where(lax.broadcasted_iota(jnp.int32, (rows - n_pair, LANES), 1) < wide, value[:rows - n_pair], value[n_pair:])
                value = jnp.concatenate([both, value[rows - n_pair:n_pair]], axis=0) if rows < 2 * n_pair else both
            n_row = min(rows, n_pair)
            flat[pl.ds(step * GROUP + s, n_row, stride=pitch), :] = value

    for_group_rows(info, first, n_frames, rows_body)

    @pl.when(step == pl.num_programs(0) - 1)
    def _():
        side = side_ref[...]
        aux_ref[...] = jnp.where(info[HALF, 0] == 0, side, pltpu.roll(side, n_own, 1))[:, :n_own]
        def flip(t, carry):
            turned = pair_ref[t, :n_own, :].T
            lp_ref[t] = turned[:n_lab + SUBS, :]
            lp_ref[t + n_pair] = turned[wide:wide + n_lab + SUBS, :]
            return carry

        lax.fori_loop(0, n_pair, flip, 0, unroll=4)
        tile = (SUBS, n_own)
        sub = lax.broadcasted_iota(jnp.int32, tile, 0)
        in_len = aux_ref[n_lab:n_lab + SUBS, :]
        lab_len = aux_ref[n_lab + SUBS:n_lab + 2 * SUBS, :]
        in_len_row = aux_ref[n_lab:n_lab + 1, :]
        neg = jnp.full(tile, NEG_FILL, jnp.float32)
        rows_of = lambda j: slice(j * SUBS, (j + 1) * SUBS)

        def forward(t, carry):
            labels, blanks, start = carry
            live = t < in_len
            tail = lp_ref[t, n_lab:n_lab + SUBS, :]
            e_blank = jnp.broadcast_to(tail[0:1, :], tile)
            new_labels, new_blanks = [], []
            for j in range(n_j):
                e_lab = lp_ref[t, rows_of(j), :]
                bias = jnp.where(aux_ref[rows_of(j), :] != 0, 0.0, NEG_FILL)
                if j:
                    one, two = blanks[j - 1], labels[j - 1]
                else:
                    one = jnp.where(sub == 0, start, pltpu.roll(blanks[n_j - 1], 1, 0))
                    two = jnp.where(sub == 0, NEG_FILL, pltpu.roll(labels[n_j - 1], 1, 0))
                two = two + bias
                top = jnp.maximum(jnp.maximum(labels[j], one), two)
                e0, e1, e2 = jnp.exp(labels[j] - top), jnp.exp(one - top), jnp.exp(two - top)
                total = e0 + e1 + e2
                inv = jnp.where(live, 1.0 / total, 0.0)
                wts[0, t, rows_of(j), :] = jnp.where(live, e0 * inv, 1.0)
                wts[1, t, rows_of(j), :] = e1 * inv
                wts[2, t, rows_of(j), :] = e2 * inv
                new_labels.append(jnp.where(live, (top + jnp.log(total)) + e_lab, labels[j]))
                top = jnp.maximum(blanks[j], labels[j])
                e0, e1 = jnp.exp(blanks[j] - top), jnp.exp(labels[j] - top)
                total = e0 + e1
                inv = jnp.where(live, 1.0 / total, 0.0)
                wts[3, t, rows_of(j), :] = jnp.where(live, e0 * inv, 1.0)
                wts[4, t, rows_of(j), :] = e1 * inv
                new_blanks.append(jnp.where(live, (top + jnp.log(total)) + e_blank, blanks[j]))
            return new_labels, new_blanks, jnp.where(t < in_len_row, start + tail[0:1, :], start)

        labels, blanks, start = lax.fori_loop(0, n_frames, forward, ([neg] * n_j, [neg] * n_j, jnp.zeros((1, n_own), jnp.float32)), unroll=2)
        end = lab_len - 1
        is_end = [sub * n_j + j == end for j in range(n_j)]
        top = neg
        for j in range(n_j):
            top = jnp.maximum(top, jnp.where(is_end[j], jnp.maximum(labels[j], blanks[j]), NEG_FILL))
        top = jnp.max(top, axis=0, keepdims=True)
        g_labels = [jnp.where(is_end[j], jnp.exp(labels[j] - top), 0.0) for j in range(n_j)]
        g_blanks = [jnp.where(is_end[j], jnp.exp(blanks[j] - top), 0.0) for j in range(n_j)]
        total = jnp.sum(sum(g_labels) + sum(g_blanks), axis=0, keepdims=True)
        loss = jnp.broadcast_to(-(top + jnp.log(total)), tile)
        inv = 1.0 / total

        def backward(i, carry):
            g_lab, g_blk, g_start = carry
            t = n_frames - 1 - i
            live = t < in_len
            for j in range(n_j):
                lp_ref[t, rows_of(j), :] = jnp.where(live, g_lab[j], 0.0)
            blank = jnp.sum(sum(g_blk), axis=0, keepdims=True) + g_start
            blank = jnp.where(t < in_len_row, blank, 0.0)
            tail = lp_ref[t, n_lab:n_lab + SUBS, :]
            lp_ref[t, n_lab:n_lab + SUBS, :] = jnp.where(sub == 0, blank, jnp.where(sub == 1, tail, jnp.where(sub == 2, loss, 0.0)))
            to_one = [g_lab[j] * wts[1, t, rows_of(j), :] for j in range(n_j)]
            to_two = [g_lab[j] * wts[2, t, rows_of(j), :] for j in range(n_j)]
            next_one = to_one[1:] + [jnp.where(sub == SUBS - 1, 0.0, pltpu.roll(to_one[0], SUBS - 1, 0))]
            next_two = to_two[1:] + [jnp.where(sub == SUBS - 1, 0.0, pltpu.roll(to_two[0], SUBS - 1, 0))]
            new_lab, new_blk = [], []
            for j in range(n_j):
                new_lab.append(g_lab[j] * wts[0, t, rows_of(j), :] + g_blk[j] * wts[4, t, rows_of(j), :] + next_two[j])
                new_blk.append(g_blk[j] * wts[3, t, rows_of(j), :] + next_one[j])
            return new_lab, new_blk, g_start + to_one[0][0:1, :]

        lax.fori_loop(0, n_frames, backward, ([g * inv for g in g_labels], [g * inv for g in g_blanks], jnp.zeros((1, n_own), jnp.float32)), unroll=2)

        def flip_back(t, carry):
            fill = jnp.zeros((wide - n_lab - SUBS, n_own), jnp.float32)
            pair_ref[t, :n_own, :] = jnp.concatenate([lp_ref[t], fill, lp_ref[t + n_pair], fill], axis=0).T
            return carry

        n_part = out_sem.shape[0]
        part = n_pair // n_part
        copies = []
        for c in range(n_part):
            lax.fori_loop(c * part, (c + 1) * part, flip_back, 0, unroll=4)
            copies.append(pltpu.make_async_copy(pair_ref.at[pl.ds(c * part, part), pl.ds(0, n_own)], occ_hbm.at[pl.ds(c * part, part)], out_sem.at[c]))
            copies[-1].start()
        for copy in copies:
            copy.wait()


def grad_kernel(is_first, info, *refs):
    enc_refs, refs = refs[:GROUP], refs[GROUP:]
    w_ref, wt_ref, occ_ref, lab_ref = refs[:4]
    if is_first:
        hs_hbm, gw_ref, loss_ref = refs[4:7]
    else:
        _, gw_in_ref, loss_in_ref, hs_hbm, gw_ref, loss_ref = refs[4:10]
    g_ref, hs_ref, acc_ref, part_ref, lse_ref, hot_ref, hs_sem = refs[-7:]
    step = pl.program_id(0)
    n_step = pl.num_programs(0)
    n_frames = enc_refs[0].shape[1]
    n_hid, n_cols = w_ref.shape
    n_chunk = 256
    wide = LANES // 2
    n_lab = lab_ref.shape[0] - 3 * SUBS
    n_pair, n_own = occ_ref.shape[:2]
    flat = occ_ref.reshape(n_pair * n_own, LANES)
    half = info[HALF, 0] if is_first else 1 - info[HALF, 0]
    slot = lax.rem(step, 2)

    def prepare(at):
        to = lax.rem(at, 2)
        left = lax.broadcasted_iota(jnp.int32, (n_frames, LANES), 1) < wide
        frame = lax.broadcasted_iota(jnp.int32, (n_frames, LANES), 0)
        for s in range(GROUP):
            occ = flat[pl.ds(at * GROUP + s, n_pair, stride=n_own), :]
            occ = jnp.concatenate([occ, pltpu.roll(occ, wide, 1)], axis=0)
            live = frame < info[LENGTH, half * n_own + at * GROUP + s]
            lse_ref[to, s] = jnp.where(live, jnp.broadcast_to(occ[:, n_lab + 1:n_lab + 2], occ.shape), -NEG_FILL)
            occ = jnp.where(live & left, occ, 0.0)
            high = occ.astype(jnp.bfloat16).astype(jnp.float32)
            rest = occ - high
            mid = rest.astype(jnp.bfloat16).astype(jnp.float32)
            part_ref[to, s, :, :LANES] = (high + pltpu.roll(mid, wide, 1)).astype(jnp.bfloat16)
            part_ref[to, s, :, LANES:] = (rest - mid).astype(jnp.bfloat16)
            hot_ref[to, s] = one_hot_rows(column(lab_ref[:wide, :], half * n_own + at * GROUP + s), n_cols)

    @pl.when(step == 0)
    def _():
        acc_ref[...] = jnp.zeros_like(acc_ref)
        prepare(0)

    def out_copy(at, s):
        seq = info[ORDER, (half * n_step + at) * GROUP + s]
        where = lax.rem(at, 2)
        return pltpu.make_async_copy(hs_ref.at[where, s], hs_hbm.at[seq], hs_sem.at[where, s])

    @pl.when(step >= 2)
    def _():
        for s in range(GROUP):
            out_copy(step - 2, s).wait()

    def rows_body(rows):
        enc = stack_rows(enc_refs, rows)
        empty = jnp.zeros((wide, n_chunk), jnp.bfloat16)
        for c in range(0, n_cols, n_chunk):
            z = dot(enc, w_ref[:, c:c + n_chunk])
            for s in range(GROUP):
                lse = lse_ref[slot, s, :rows, :]
                prob = jnp.exp(z[s * rows:(s + 1) * rows] - jnp.concatenate([lse] * (n_chunk // LANES), axis=1))
                hot = hot_ref[slot, s, :, c:c + n_chunk]
                spread = dot(part_ref[slot, s, :rows, :], jnp.concatenate([hot, hot, hot, empty], axis=0))
                g_ref[s * rows:(s + 1) * rows, c:c + n_chunk] = (prob - spread).astype(jnp.bfloat16)
        prepare(jnp.minimum(step + 1, n_step - 1))
        grad = dot(g_ref[:GROUP * rows, :], wt_ref[...])
        for s in range(GROUP):
            hs_ref[slot, s, :rows, :] = grad[s * rows:(s + 1) * rows]
            if rows < n_frames:
                hs_ref[slot, s, rows:, :] = jnp.zeros((n_frames - rows, n_hid), jnp.float32)
        mine = g_ref[:GROUP * rows, pl.ds(pl.multiple_of(info[INDEX, 0] * LANES, LANES), LANES)]
        acc_ref[...] += lax.dot_general(mine, enc, (((0,), (0,)), ((), ())), preferred_element_type=jnp.float32)

    for_group_rows(info, half * n_own + step * GROUP, n_frames, rows_body)
    for s in range(GROUP):
        out_copy(step, s).start()

    @pl.when(step == n_step - 1)
    def _():
        total = acc_ref[...].T
        gw_ref[...] = total if is_first else total + gw_in_ref[...]
        loss = occ_ref[0, :, n_lab + 2:n_lab + 3]
        sub = lax.broadcasted_iota(jnp.int32, (n_own, LANES), 0) + half * n_own
        lane_slot = lab_ref[wide:wide + 1, :]
        loss = jnp.sum(jnp.where(sub == lane_slot, loss, 0.0), axis=0, keepdims=True)
        loss_ref[...] = loss if is_first else loss + loss_in_ref[...]
        for back in (1, 0):
            for s in range(GROUP):
                out_copy(step - back, s).wait()


def exact_dot(a, b, dims):
    return lax.dot_general(a, b, (dims, ((), ())), precision=lax.Precision.HIGHEST, preferred_element_type=jnp.float32)


def sort_tables(labels, lens, index):
    n_batch, n_lab = labels.shape
    n_j = n_lab // SUBS
    square = (n_batch, n_batch)
    row = lax.broadcasted_iota(jnp.int32, square, 0)
    col = lax.broadcasted_iota(jnp.int32, square, 1)
    along = lambda values: jnp.broadcast_to(values.astype(jnp.float32), square)
    in_cols, lab_rows = along(lens[0:1]), along(lens[1:2]).T
    in_rows = in_cols.T
    ahead = (in_cols > in_rows) | ((in_cols == in_rows) & (col < row))
    rank = jnp.sum(ahead.astype(jnp.int32), axis=1, keepdims=True)
    slot = (rank & 1) * (n_batch // 2) + (rank >> 1)
    at_slot = col == slot
    pick = lambda values: jnp.sum(jnp.where(at_slot, values, 0.0), axis=0, keepdims=True).astype(jnp.int32)
    in_sorted, lab_sorted = pick(in_rows), pick(lab_rows)
    slot_row = along(slot).T[0:1].astype(jnp.int32)
    half = lax.rem(index, 2)
    fill = lambda value: jnp.broadcast_to(value, (1, n_batch))
    info = jnp.concatenate([pick(row.astype(jnp.float32)), in_sorted, slot_row, fill(half), fill(index)] + [fill(0)] * 3, axis=0)

    lab = lax.broadcasted_iota(jnp.int32, (n_lab, LANES), 0)
    to = lax.broadcasted_iota(jnp.int32, (n_lab, LANES), 1) % (LANES // 2)
    source = (to % SUBS) * n_j + to // SUBS
    inside = to < n_lab
    values = labels.astype(jnp.float32)
    here = exact_dot(values, jnp.where(inside & (lab == source), 1.0, 0.0), ((1,), (0,)))
    before = exact_dot(values, jnp.where(inside & (lab == source - 1), 1.0, 0.0), ((1,), (0,)))
    to = lax.broadcasted_iota(jnp.int32, (n_batch, LANES), 1) % (LANES // 2)
    skip = jnp.where((here != before) & (to % SUBS * n_j + to // SUBS > 0), 1.0, 0.0)
    here = jnp.where(to > n_lab, -1.0, here)
    mix = jnp.where(at_slot, 1.0, 0.0)
    lab_rows = exact_dot(mix, here, ((0,), (0,)))
    skip_cols = exact_dot(mix, skip, ((0,), (0,))).T.astype(jnp.int32)
    side = jnp.concatenate([skip_cols[:n_lab], jnp.broadcast_to(in_sorted, (SUBS, n_batch)), jnp.broadcast_to(lab_sorted, (SUBS, n_batch))], axis=0)
    lab_cols = jnp.concatenate([lab_rows.T[:LANES // 2].astype(jnp.int32), jnp.broadcast_to(slot_row, (SUBS, n_batch))], axis=0)
    return info, lab_rows.astype(jnp.int32), lab_cols, side


def gather_kernel(n_group, w_ref, labels_ref, lens_ref, w_all_ref, wt_all_ref, info_ref, lab_rows_ref, lab_cols_ref, side_ref,
                  got_ref, send_sem, recv_sem):
    me = lax.axis_index("tp")
    n_hid, n_local = w_ref.shape
    mid = n_hid // 2
    other = me + 1 - 2 * lax.rem(me, 2)
    right = lax.rem(me + 2, n_group)
    back = lax.rem(me + n_group - 2, n_group)
    far = lax.rem(me + n_group // 2, n_group)

    barrier = pltpu.get_barrier_semaphore()
    for peer in (other, right, back):
        pl.semaphore_signal(barrier, inc=1, device_id={"tp": peer}, device_id_type=pl.DeviceIdType.MESH)
    pl.semaphore_wait(barrier, 3)

    def send(k, src, dst, peer):
        copy = pltpu.make_async_remote_copy(src_ref=src, dst_ref=dst, send_sem=send_sem.at[k], recv_sem=recv_sem.at[k],
                                            device_id={"tp": peer}, device_id_type=pl.DeviceIdType.MESH)
        copy.start()
        return copy

    def place(block, values):
        at = pl.ds(pl.multiple_of(block * n_local, n_local), n_local)
        w_all_ref[:, at] = values
        wt_all_ref[at, :] = values.T

    flip = lambda block: block + 1 - 2 * lax.rem(block, 2)
    copies = [send(0, w_ref, got_ref.at[me], right), send(1, w_ref, got_ref.at[me], back), send(2, w_ref, got_ref.at[me], other)]
    place(me, w_ref[...])
    info_ref[...], lab_rows_ref[...], lab_cols_ref[...], side_ref[...] = sort_tables(labels_ref[...], lens_ref[...], me)
    copies[0].wait_recv()
    copies.append(send(3, got_ref.at[back, pl.ds(0, mid)], got_ref.at[back, pl.ds(0, mid)], right))
    copies.append(send(4, got_ref.at[back], got_ref.at[back], other))
    copies[1].wait_recv()
    copies.append(send(5, got_ref.at[right, pl.ds(mid, mid)], got_ref.at[right, pl.ds(mid, mid)], back))
    copies.append(send(6, got_ref.at[right], got_ref.at[right], other))
    place(back, got_ref[back])
    place(right, got_ref[right])
    copies[2].wait_recv()
    place(other, got_ref[other])
    copies[4].wait_recv()
    place(flip(back), got_ref[flip(back)])
    copies[6].wait_recv()
    place(flip(right), got_ref[flip(right)])
    copies[3].wait_recv()
    copies.append(send(7, got_ref.at[far, pl.ds(0, mid)], got_ref.at[far, pl.ds(0, mid)], other))
    copies[5].wait_recv()
    copies.append(send(8, got_ref.at[far, pl.ds(mid, mid)], got_ref.at[far, pl.ds(mid, mid)], other))
    place(far, got_ref[far])
    copies[7].wait_recv()
    copies[8].wait_recv()
    place(flip(far), got_ref[flip(far)])
    for copy in copies:
        copy.wait_send()


def run_gather(w_loc, labels, lens, n_group):
    n_hid, n_local = w_loc.shape
    n_cols = n_local * n_group
    n_batch, n_lab = labels.shape
    vmem = pl.BlockSpec(memory_space=pltpu.VMEM)
    table = lambda *dims: jax.ShapeDtypeStruct(dims, jnp.int32)
    return pl.pallas_call(
        functools.partial(gather_kernel, n_group),
        in_specs=[vmem] * 3,
        out_specs=[vmem] * 6,
        out_shape=[
            jax.ShapeDtypeStruct((n_hid, n_cols), w_loc.dtype),
            jax.ShapeDtypeStruct((n_cols, n_hid), w_loc.dtype),
            table(SUBS, n_batch),
            table(n_batch, LANES),
            table(LANES // 2 + SUBS, n_batch),
            table(n_lab + 2 * SUBS, n_batch),
        ],
        scratch_shapes=[pltpu.VMEM((n_group, n_hid, n_local), w_loc.dtype), pltpu.SemaphoreType.DMA((9,)), pltpu.SemaphoreType.DMA((9,))],
        compiler_params=pltpu.CompilerParams(collective_id=0, has_side_effects=True, vmem_limit_bytes=VMEM_BYTES),
        name="gather",
    )(w_loc, labels, lens)


def whole(*dims):
    return pl.BlockSpec(dims, lambda i, info: (0,) * len(dims))


def enc_specs(n_step, n_frames, n_hid, swap=False):
    def spec(s):
        def where(i, info):
            half = 1 - info[HALF, 0] if swap else info[HALF, 0]
            return info[ORDER, (half * n_step + i) * GROUP + s], 0, 0
        return pl.BlockSpec((1, n_frames, n_hid), where)
    return [spec(s) for s in range(GROUP)]


def run_lattice(info, enc_out, w_all, lab_rows, side):
    n_batch, n_frames, n_hid = enc_out.shape
    n_own = n_batch // 2
    n_cols = w_all.shape[1]
    n_step = n_own // GROUP
    n_side = side.shape[0]
    n_lab = n_side - 2 * SUBS
    return pl.pallas_call(
        functools.partial(lattice_kernel, n_own),
        grid_spec=pltpu.PrefetchScalarGridSpec(
            num_scalar_prefetch=1,
            grid=(n_step,),
            in_specs=enc_specs(n_step, n_frames, n_hid) + [whole(n_hid, n_cols), whole(*lab_rows.shape), whole(*side.shape)],
            out_specs=pl.BlockSpec(memory_space=pl.ANY),
            scratch_shapes=[
                pltpu.VMEM((5, n_frames, n_lab, n_own), jnp.float32),
                pltpu.VMEM((GROUP * n_frames, n_cols), jnp.float32),
                pltpu.VMEM((n_frames // 2, n_own + SUBS, LANES), jnp.float32),
                pltpu.VMEM((n_frames, n_lab + SUBS, n_own), jnp.float32),
                pltpu.VMEM((n_side, n_own), jnp.int32),
                pltpu.SemaphoreType.DMA((4,)),
            ],
        ),
        out_shape=jax.ShapeDtypeStruct((n_frames // 2, n_own, LANES), jnp.float32),
        compiler_params=pltpu.CompilerParams(vmem_limit_bytes=VMEM_BYTES),
        name="lattice",
    )(info, *[enc_out] * GROUP, w_all, lab_rows, side)


def run_grad(info, enc_out, w_all, wt_all, occ, lab_cols, n_local, prior=None):
    n_batch, n_frames, n_hid = enc_out.shape
    n_cols = w_all.shape[1]
    n_step = occ.shape[1] // GROUP
    is_first = prior is None
    in_specs = enc_specs(n_step, n_frames, n_hid, not is_first) + [
        whole(n_hid, n_cols),
        whole(n_cols, n_hid),
        whole(*occ.shape),
        whole(*lab_cols.shape),
    ]
    operands = [info] + [enc_out] * GROUP + [w_all, wt_all, occ, lab_cols]
    aliases = {}
    if not is_first:
        aliases = {len(operands): 0}
        in_specs += [pl.BlockSpec(memory_space=pl.ANY), whole(n_hid, n_local), whole(1, n_batch)]
        operands += list(prior)
    return pl.pallas_call(
        functools.partial(grad_kernel, is_first),
        grid_spec=pltpu.PrefetchScalarGridSpec(
            num_scalar_prefetch=1,
            grid=(n_step,),
            in_specs=in_specs,
            out_specs=[pl.BlockSpec(memory_space=pl.ANY), whole(n_hid, n_local), whole(1, n_batch)],
            scratch_shapes=[
                pltpu.VMEM((GROUP * n_frames, n_cols), jnp.bfloat16),
                pltpu.VMEM((2, GROUP, n_frames, n_hid), jnp.float32),
                pltpu.VMEM((n_local, n_hid), jnp.float32),
                pltpu.VMEM((2, GROUP, n_frames, 2 * LANES), jnp.bfloat16),
                pltpu.VMEM((2, GROUP, n_frames, LANES), jnp.float32),
                pltpu.VMEM((2, GROUP, LANES // 2, n_cols), jnp.bfloat16),
                pltpu.SemaphoreType.DMA((2, GROUP)),
            ],
        ),
        out_shape=[
            jax.ShapeDtypeStruct((n_batch, n_frames, n_hid), jnp.float32),
            jax.ShapeDtypeStruct((n_hid, n_local), jnp.float32),
            jax.ShapeDtypeStruct((1, n_batch), jnp.float32),
        ],
        input_output_aliases=aliases,
        compiler_params=pltpu.CompilerParams(vmem_limit_bytes=VMEM_BYTES),
        cost_estimate=pl.CostEstimate(flops=3 * n_batch * n_frames * n_hid * n_cols, bytes_accessed=50_000_000, transcendentals=0),
        name="grad_first" if is_first else "grad_second",
    )(*operands)


def solution(mesh):
    n_group = mesh.shape["tp"]

    def device_fn(enc_out, w_loc, labels, in_len, lab_len):
        w_all, wt_all, info, lab_rows, lab_cols, side = run_gather(w_loc, labels, jnp.stack([in_len, lab_len]), n_group)
        occ = run_lattice(info, enc_out, w_all, lab_rows, side)
        occ_other = lax.ppermute(occ, "tp", [(i, i ^ 1) for i in range(n_group)])
        prior = run_grad(info, enc_out, w_all, wt_all, occ, lab_cols, w_loc.shape[1])
        grad_hs, grad_w, loss = run_grad(info, enc_out, w_all, wt_all, occ_other, lab_cols, w_loc.shape[1], prior)
        return loss[0], grad_w, grad_hs

    return jax.shard_map(device_fn, mesh=mesh, in_specs=(P("dp"), P(None, "tp"), P("dp"), P("dp"), P("dp")), out_specs=(P("dp"), P("dp", "tp"), P("dp")), check_vma=False)
```
